32 devices in a mesh: grp: 4 (over z), kv: 4 (over y, x), tp: 2 (over core).
Axes of the slice: x: 2, y: 2, z: 4, core: 2. Of those that a mesh axis runs over, the one named last changes fastest.
Arguments:
- hidden_states: bfloat16 [512, 4096], P('grp', 'kv'), may hold values from -6 to 6
- attn_gain: float32 [4096], P('kv'), may hold values from 0.25 to 1.75
- mlp_gain: float32 [4096], replicated, may hold values from 0.25 to 1.75
- w_query: bfloat16 [4096, 4096], P('kv', 'tp'), may hold values from -0.09375 to 0.09375
- w_out: bfloat16 [32, 128, 4096], P('tp', 'kv'), may hold values from -1 to 1
- w_gate: bfloat16 [4096, 14336], P(None, ('kv', 'tp')), may hold values from -0.09375 to 0.09375
- w_up: bfloat16 [4096, 14336], P(None, ('kv', 'tp')), may hold values from -0.09375 to 0.09375
- w_down: bfloat16 [14336, 4096], P(('kv', 'tp')), may hold values from -0.046875 to 0.046875
- kv_pool: bfloat16 [256, 2, 128, 1024], P(('grp', 'kv'), None, None, 'tp'), may hold values from -110 to 110
- resident_cache: bfloat16 [4, 32, 2, 128, 1024], P('grp', 'kv', None, None, 'tp'), may hold values from -110 to 110
- resident_slot: int32 [4, 32], P('grp', 'kv'), may hold values from 0 to 127
- resident_len: int32 [4, 32], P('grp', 'kv'), may hold values from 1 to 128
- new_owner: int32 [4, 64], replicated, may hold values from 0 to 15, as said below
- new_local: int32 [4, 64], replicated, may hold values from 0 to 15
- new_slot: int32 [4, 64], P('grp', 'kv'), may hold values from 0 to 127
- new_len: int32 [4, 64], P('grp', 'kv'), may hold values from 1 to 128
- token_kv: bfloat16 [512, 2, 1024], P('grp', None, 'tp'), may hold values from -6 to 6
Outputs:
- mixed: bfloat16 [512, 4096], P(('grp', 'kv', 'tp'))
- new_cache: bfloat16 [4, 64, 2, 128, 1024], P('grp', 'kv', None, None, 'tp')
The draws below stay inside these ranges and needn't reach their ends.
Inputs may be any that keep to these rules, and one draw needn't show every extreme that they name: New page c of group g is kept by the device of kv index c // 16 of group g and comes from the device whose index along grp+kv is new_owner[g, c]; every decode device receives exactly 4 new pages from the owners of each grp index; no owner sends more than 4 pages to the devices of one kv index over all groups, so at most 4 to one device; every owner sends each of its 16 pages exactly once.
All inputs are finite; a program needn't handle non-finite values.
Results may differ from the reference program's by a relative error of at most 0.018.
Values may be sent and summed in bfloat16 or wider, within the bound.
No kernel may reach another device: no remote copies, remote signals or barrier semaphores. Data moves between devices by JAX's collectives and lax.ppermute only.
A program may use at most 128 MiB of HBM per device.

```python
import jax
import jax.numpy as jnp
from jax import lax

D = 4096
HEADS = 32
KV_HEADS = 8
HEAD_DIM = 128
FF = 14336
PAGE = 128
NPR = 4
SLOT_G = 128
GROUPS = 4
KV_RANKS = 4
SLOTS = 512
NEW_DEV = 16
CAP1 = 4
POOL = 256
CACHE_G = 32
NEWC = 64


def page_values(key, count):
    width = KV_HEADS * HEAD_DIM
    values = jnp.clip(jax.random.normal(key, (count, 2, PAGE, width), jnp.float32), -6.0, 6.0)
    return values.astype(jnp.bfloat16)


def draw_kv_pool(key, part):
    return page_values(jax.random.fold_in(key, 3), POOL)


def draw_resident_cache(key, part):
    values = page_values(jax.random.fold_in(key, 5), GROUPS * CACHE_G)
    return values.reshape(GROUPS, CACHE_G, 2, PAGE, KV_HEADS * HEAD_DIM)


def batch_perms(key, count, length):
    subkeys = jax.random.split(key, count)
    return jax.vmap(lambda subkey: jax.random.permutation(subkey, length))(subkeys)


def route_tables(key):
    key = jax.random.fold_in(key, 11)
    keys = jax.random.split(key, 4)
    cap = CAP1
    col_perm = batch_perms(keys[0], GROUPS * KV_RANKS, KV_RANKS).reshape(GROUPS, KV_RANKS, KV_RANKS)
    shift = jax.random.randint(keys[1], (GROUPS, KV_RANKS), 0, KV_RANKS)
    dest_perm = batch_perms(keys[2], GROUPS * KV_RANKS, NEW_DEV).reshape(GROUPS, KV_RANKS, NEW_DEV)
    local_perm = batch_perms(keys[3], GROUPS * KV_RANKS, NEW_DEV)
    src_grp = jnp.arange(GROUPS).reshape(GROUPS, 1, 1, 1)
    dst_col = jnp.arange(KV_RANKS).reshape(1, KV_RANKS, 1, 1)
    dst_grp = jnp.arange(GROUPS).reshape(1, 1, GROUPS, 1)
    within = jnp.arange(NPR).reshape(1, 1, 1, NPR)
    flat = dst_grp * NPR + within
    turned = (flat + shift[src_grp, dst_col] * cap) % NEW_DEV
    block = turned // cap
    place = turned % cap
    src_col = col_perm[src_grp, dst_col, block]
    owner = src_grp * KV_RANKS + src_col
    local_ids = local_perm[owner, dst_col * cap + place]
    slot_in = dest_perm[dst_grp, dst_col, src_grp * NPR + within]
    column = dst_col * NEW_DEV + slot_in
    full_rows = jnp.broadcast_to(dst_grp, owner.shape)
    owners = jnp.zeros((GROUPS, KV_RANKS * NEW_DEV), jnp.int32).at[full_rows, column].set(owner.astype(jnp.int32))
    locals_out = jnp.zeros((GROUPS, KV_RANKS * NEW_DEV), jnp.int32).at[full_rows, column].set(local_ids.astype(jnp.int32))
    return (owners, locals_out)


def draw_new_owner(key, part):
    return route_tables(key)[0]


def draw_new_local(key, part):
    return route_tables(key)[1]


def set_ends(drawn, key, least, high):
    longest = drawn.shape.index(max(drawn.shape))
    spots = []
    for shift in (0, 1):
        where = [jax.random.randint(jax.random.fold_in(key, axis), (), 0, length) for axis, length in enumerate(drawn.shape)]
        where[longest] = (where[longest] + shift) % drawn.shape[longest]
        spots.append(tuple(where))
    return drawn.at[spots[0]].set(least).at[spots[1]].set(high)


def block_levels(key, dims, shards, smallest, largest):
    factor_of, own = 1.0, jax.random.fold_in(key, 6)
    for position, blocks in shards:
        steps = jnp.exp(jax.random.uniform(jax.random.fold_in(own, position), (blocks,), jnp.float32, smallest / len(shards), largest / len(shards)))
        factor_of = factor_of * jnp.repeat(steps, dims[position] // blocks).reshape([-1 if axis == position else 1 for axis in range(len(dims))])
    return factor_of


def gaussian(stream_key, shape, spread, most, pieces=(), held_as=jnp.bfloat16):
    values = spread * jax.random.normal(stream_key, shape, jnp.float32)
    if pieces:
        values = values * block_levels(stream_key, shape, pieces, -0.22, 0.18)
    return jnp.clip(values, -most, most).astype(held_as)


def setup_inputs(seed: int = 0) -> dict:
    key_list = jax.random.split(jax.random.key(seed), 18)
    return {
        "hidden_states": gaussian(key_list[0], (SLOTS, D), 1.0, 6.0, ((0, 4), (1, 4))),
        "attn_gain": jnp.clip(1.0 + 0.15 * jax.random.normal(key_list[1], (D,), jnp.float32), 0.25, 1.75),
        "mlp_gain": jnp.clip(1.0 + 0.15 * jax.random.normal(key_list[2], (D,), jnp.float32), 0.25, 1.75),
        "w_query": gaussian(key_list[3], (D, HEADS * HEAD_DIM), D ** -0.5, 0.09375, ((0, 4), (1, 2))),
        "w_out": gaussian(key_list[4], (HEADS, HEAD_DIM, D), HEADS ** -0.5, 1.0, ((0, 2), (1, 4))),
        "w_gate": gaussian(key_list[5], (D, FF), D ** -0.5, 0.09375, ((1, 8),)),
        "w_up": gaussian(key_list[6], (D, FF), D ** -0.5, 0.09375, ((1, 8),)),
        "w_down": gaussian(key_list[7], (FF, D), FF ** -0.5, 0.046875, ((0, 8),)),
        "kv_pool": draw_kv_pool(jax.random.fold_in(key_list[17], 71), 0),
        "resident_cache": draw_resident_cache(jax.random.fold_in(key_list[17], 71), 0),
        "resident_slot": set_ends(jax.random.randint(key_list[10], (GROUPS, CACHE_G), 0, SLOT_G), jax.random.fold_in(key_list[10], 1), 0, SLOT_G - 1).astype(jnp.int32),
        "resident_len": set_ends(jax.random.randint(key_list[11], (GROUPS, CACHE_G), 1, PAGE + 1), jax.random.fold_in(key_list[11], 1), 1, PAGE).astype(jnp.int32),
        "new_owner": draw_new_owner(jax.random.fold_in(key_list[17], 71), 0),
        "new_local": draw_new_local(jax.random.fold_in(key_list[17], 71), 0),
        "new_slot": set_ends(jax.random.randint(key_list[14], (GROUPS, NEWC), 0, SLOT_G), jax.random.fold_in(key_list[14], 1), 0, SLOT_G - 1).astype(jnp.int32),
        "new_len": set_ends(jax.random.randint(key_list[15], (GROUPS, NEWC), 1, PAGE + 1), jax.random.fold_in(key_list[15], 1), 1, PAGE).astype(jnp.int32),
        "token_kv": gaussian(key_list[16], (SLOTS, 2, KV_HEADS * HEAD_DIM), 1.0, 6.0, ((0, 4), (2, 2))),
    }


neg_fill = -1e+30
norm_eps = 1e-05

def local_partials(query, resident, arrived, res_slot, res_len, arr_slot, arr_len, token_kv, first):
    pages = jnp.concatenate([resident, arrived], axis=0)
    owner_slot = jnp.concatenate([res_slot, arr_slot]).astype(jnp.int32)
    filled = jnp.concatenate([res_len, arr_len]).astype(jnp.int32)
    count = pages.shape[0]
    tokens = pages.shape[2]
    kv_here = pages.shape[3] // HEAD_DIM
    slots = query.shape[0]
    ratio = HEADS // KV_HEADS
    keys = pages[:, 0].astype(jnp.float32).reshape(count, tokens, kv_here, HEAD_DIM)
    values = pages[:, 1].astype(jnp.float32).reshape(count, tokens, kv_here, HEAD_DIM)
    grouped = query.reshape(slots, kv_here, ratio, HEAD_DIM)
    picked = jnp.take(grouped, owner_slot, axis=0)
    scores = jnp.einsum('ikgd,itkd->ikgt', picked, keys, precision=lax.Precision.HIGHEST)
    usable = (jnp.arange(tokens, dtype=jnp.int32)[None, :] < filled[:, None])[:, None, None, :]
    scores = jnp.where(usable, scores, neg_fill)
    page_top = lax.optimization_barrier(jnp.max(scores, axis=3))
    member = owner_slot[None, :] == jnp.arange(slots, dtype=jnp.int32)[:, None]
    slot_top = lax.optimization_barrier(jnp.max(jnp.where(member[:, :, None, None], page_top[None], neg_fill), axis=1))
    own_keys = token_kv[:, 0].astype(jnp.float32).reshape(slots, kv_here, HEAD_DIM)
    own_values = token_kv[:, 1].astype(jnp.float32).reshape(slots, kv_here, HEAD_DIM)
    own_score = jnp.einsum('skgd,skd->skg', grouped, own_keys, precision=lax.Precision.HIGHEST)
    own_score = jnp.where(first, own_score, neg_fill)
    slot_top = jnp.maximum(slot_top, own_score)
    reach = jnp.take(slot_top, owner_slot, axis=0)
    weights = jnp.where(usable, jnp.exp(scores - reach[..., None]), 0.0)
    page_sum = lax.optimization_barrier(jnp.sum(weights, axis=3))
    page_acc = jnp.einsum('ikgt,itkd->ikgd', weights, values, precision=lax.Precision.HIGHEST)
    own_weight = jnp.where(first, jnp.exp(own_score - slot_top), 0.0)
    member_f = member.astype(jnp.float32)
    total = jnp.dot(member_f, page_sum.reshape(count, -1), precision=lax.Precision.HIGHEST)
    total = total + own_weight.reshape(slots, -1)
    weighted = jnp.dot(member_f, page_acc.reshape(count, -1), precision=lax.Precision.HIGHEST)
    weighted = weighted.reshape(slots, kv_here, ratio, HEAD_DIM) + own_weight[..., None] * own_values[:, :, None, :]
    return (slot_top.reshape(slots, -1), total, weighted.reshape(slots, kv_here * ratio, HEAD_DIM))

def reference(hidden_states, attn_gain, mlp_gain, w_query, w_out, w_gate, w_up, w_down, kv_pool, resident_cache, resident_slot, resident_len, new_owner, new_local, new_slot, new_len, token_kv):
    groups = SLOTS // SLOT_G
    features = hidden_states.astype(jnp.float32)
    attn_scale = lax.rsqrt(lax.optimization_barrier(jnp.sum(features * features, axis=1)) / D + norm_eps)
    normed = (features * attn_gain).astype(jnp.bfloat16)
    query = jnp.dot(normed, w_query, preferred_element_type=jnp.float32) * attn_scale[:, None] * HEAD_DIM ** (-0.5)
    index = (new_owner * NEW_DEV + new_local).reshape(-1).astype(jnp.int32)
    new_cache = jnp.take(kv_pool, index, axis=0).reshape(groups, NEWC, 2, PAGE, KV_HEADS * HEAD_DIM)

    def attend(packed):
        grp_query, resident, arrived, res_slot, res_len, arr_slot, arr_len, own_kv = packed
        top, total, weighted = local_partials(grp_query, resident, arrived, res_slot, res_len, arr_slot, arr_len, own_kv, True)
        return (weighted / total[..., None]).astype(jnp.bfloat16)
    attn = lax.map(attend, (query.reshape(groups, SLOT_G, HEADS * HEAD_DIM), resident_cache, new_cache, resident_slot, resident_len, new_slot, new_len, token_kv.reshape(groups, SLOT_G, 2, KV_HEADS * HEAD_DIM)))
    attn = attn.reshape(SLOTS, HEADS * HEAD_DIM)
    branch = jnp.dot(attn, w_out.reshape(HEADS * HEAD_DIM, D), preferred_element_type=jnp.float32)
    resid = (features + branch).astype(jnp.bfloat16)
    resid_f = resid.astype(jnp.float32)
    mlp_scale = lax.rsqrt(lax.optimization_barrier(jnp.sum(resid_f * resid_f, axis=1)) / D + norm_eps)
    normed_mlp = (resid_f * mlp_gain).astype(jnp.bfloat16)
    gate = jnp.dot(normed_mlp, w_gate, preferred_element_type=jnp.float32) * mlp_scale[:, None]
    upward = jnp.dot(normed_mlp, w_up, preferred_element_type=jnp.float32) * mlp_scale[:, None]
    hidden_units = (jax.nn.silu(gate) * upward).astype(jnp.bfloat16)
    mixed = (resid_f + jnp.dot(hidden_units, w_down, preferred_element_type=jnp.float32)).astype(jnp.bfloat16)
    return (mixed, new_cache)
```

```python
import functools

import jax
import jax.numpy as jnp
from jax import lax
from jax.experimental import pallas as pl
from jax.experimental.pallas import tpu as pltpu
from jax.sharding import PartitionSpec as P

D = 4096
HEAD_DIM = 128
norm_eps = 1e-05
neg_fill = -1e30
f32, bf16, i32 = jnp.float32, jnp.bfloat16, jnp.int32
ANY = pl.BlockSpec(memory_space=pl.ANY)
SMEM = pl.BlockSpec(memory_space=pltpu.SMEM)
VMEM = pl.BlockSpec(memory_space=pltpu.VMEM)

SHARES = (0.5, 0.5)


def after(x, dep):
    return lax.optimization_barrier((x, dep))[0]


def iota(shape, axis):
    return lax.broadcasted_iota(i32, shape, axis)


def gather_kernel(lo, size, count, idx, pool, *rest):
    outs, (buf, sem_in, sem_out) = rest[:-3], rest[-3:]
    per = count // len(outs)

    def load(j):
        src = pool.at[idx[j], :, pl.ds(lo, size), :]
        return pltpu.make_async_copy(src, buf.at[j], sem_in.at[j])

    def store(j):
        return pltpu.make_async_copy(buf.at[j], outs[j // per].at[j % per], sem_out.at[j])

    for j in range(count):
        load(j).start()
    for j in range(count):
        load(j).wait()
        store(j).start()
    for j in range(count):
        store(j).wait()


def page_gather(idx, pool, lo, size, parts):
    count = idx.shape[0]
    one = (count // parts, 2, size, pool.shape[3])
    return pl.pallas_call(
        functools.partial(gather_kernel, lo, size, count),
        out_shape=[jax.ShapeDtypeStruct(one, pool.dtype)] * parts,
        in_specs=[SMEM, ANY],
        out_specs=[ANY] * parts,
        scratch_shapes=[
            pltpu.VMEM((count, 2, size, pool.shape[3]), pool.dtype),
            pltpu.SemaphoreType.DMA((count,)),
            pltpu.SemaphoreType.DMA((count,)),
        ],
        name="page_gather",
    )(idx, pool)


def sort_kernel(count, n_in, idx, *rest):
    ins, outs = rest[:n_in], rest[n_in:-3]
    buf, sem_in, sem_out = rest[-3:]
    per_in, per_out = count // n_in, count // len(outs)

    def load(j):
        return pltpu.make_async_copy(ins[j // per_in].at[j % per_in], buf.at[j], sem_in.at[j])

    def store(j):
        dst = outs[j // per_out].at[j % per_out]
        return pltpu.make_async_copy(buf.at[idx[j]], dst, sem_out.at[j])

    for j in range(count):
        load(j).start()
    for j in range(count):
        load(j).wait()
    for j in range(count):
        store(j).start()
    for j in range(count):
        store(j).wait()


def page_sort(idx, ins, parts):
    count = idx.shape[0]
    tail = ins[0].shape[1:]
    one = (count // parts,) + tail
    return pl.pallas_call(
        functools.partial(sort_kernel, count, len(ins)),
        out_shape=[jax.ShapeDtypeStruct(one, ins[0].dtype)] * parts,
        in_specs=[SMEM] + [ANY] * len(ins),
        out_specs=[ANY] * parts,
        scratch_shapes=[
            pltpu.VMEM((count,) + tail, ins[0].dtype),
            pltpu.SemaphoreType.DMA((count,)),
            pltpu.SemaphoreType.DMA((count,)),
        ],
        name="page_sort",
    )(idx, *ins)


def place_kernel(lo, size, count, n_in, aliased, idx, *rest):
    ins = rest[:n_in]
    out = rest[n_in + (1 if aliased else 0)]
    buf, sem_in, sem_out = rest[-3:]
    per_in = count // n_in

    def load(j):
        return pltpu.make_async_copy(ins[j // per_in].at[j % per_in], buf.at[j], sem_in.at[j])

    def store(j):
        dst = out.at[j, :, pl.ds(lo, size), :]
        return pltpu.make_async_copy(buf.at[idx[j]], dst, sem_out.at[j])

    for j in range(count):
        load(j).start()
    for j in range(count):
        load(j).wait()
    for j in range(count):
        store(j).start()
    for j in range(count):
        store(j).wait()


def page_place(idx, ins, lo, whole, so_far):
    count = idx.shape[0]
    size = ins[0].shape[2]
    aliased = so_far is not None
    out = jax.ShapeDtypeStruct((count, 2, whole, ins[0].shape[3]), ins[0].dtype)
    return pl.pallas_call(
        functools.partial(place_kernel, lo, size, count, len(ins), aliased),
        out_shape=out,
        in_specs=[SMEM] + [ANY] * (len(ins) + (1 if aliased else 0)),
        out_specs=ANY,
        scratch_shapes=[
            pltpu.VMEM((count,) + ins[0].shape[1:], ins[0].dtype),
            pltpu.SemaphoreType.DMA((count,)),
            pltpu.SemaphoreType.DMA((count,)),
        ],
        input_output_aliases={len(ins) + 1: 0} if aliased else {},
        name="page_place",
    )(idx, *ins, *((so_far,) if aliased else ()))


def shifted(parts, axis):
    n = lax.axis_size(axis)
    moved = [parts[0]]
    for s in range(1, n):
        moved.append(lax.ppermute(parts[s], axis, [(i, (i + s) % n) for i in range(n)]))
    return moved


def three(x):
    hi = x.astype(bf16)
    rest = x - hi.astype(f32)
    mid = rest.astype(bf16)
    low = (rest - mid.astype(f32)).astype(bf16)
    return hi, mid, low


def attend_kernel(
    n_new, n_kept, block, span, new_len, kept_len, q_ref, own_ref, new_ref, kept_ref, out_ref, qs, acc, stat
):
    ranks, rows = q_ref.shape[0], n_new + n_kept
    heads = q_ref.shape[2] // HEAD_DIM
    width = new_ref.shape[3]
    kv_here = width // HEAD_DIM
    ratio = heads // kv_here
    step = pl.program_id(0)
    new_steps = n_new // block

    @pl.when(step == 0)
    def _():
        for h in range(heads):
            lanes = pl.ds(h * HEAD_DIM, HEAD_DIM)
            total = q_ref[0, :, lanes]
            for k in range(1, ranks):
                total = total + q_ref[k, :, lanes]
            qs[:, h, :] = total

    row_of = lax.broadcasted_iota(i32, (heads, width), 0)
    lane_of = lax.broadcasted_iota(i32, (heads, width), 1)
    own_block = (row_of // ratio) == (lane_of // HEAD_DIM)
    tok = lax.broadcasted_iota(i32, (heads, HEAD_DIM), 1)
    hrow = lax.broadcasted_iota(i32, (heads, HEAD_DIM), 0)

    def page(row, filled, keys, values):
        q = qs[row]
        wide = jnp.where(own_block, jnp.concatenate([q] * kv_here, axis=1), 0.0)
        lhs = jnp.concatenate(three(wide), axis=0)
        s3 = lax.dot_general(lhs, keys, (((1,), (1,)), ((), ())), preferred_element_type=f32)
        tokens = keys.shape[0]
        s = s3[:heads] + (s3[heads : 2 * heads] + s3[2 * heads :])
        usable = lax.broadcasted_iota(i32, (heads, tokens), 1) < filled
        s = jnp.where(usable, s, neg_fill)
        top = jnp.max(s, axis=1, keepdims=True)
        p = jnp.where(usable, jnp.exp(s - top), 0.0)
        total = jnp.sum(p, axis=1, keepdims=True)
        phi = p.astype(bf16)
        plo = (p - phi.astype(f32)).astype(bf16)
        o2 = jnp.dot(jnp.concatenate([phi, plo], axis=0), values, preferred_element_type=f32)
        o = jnp.where(own_block, o2[:heads] + o2[heads:], 0.0)
        res = o[:, :HEAD_DIM]
        for b in range(1, kv_here):
            res = res + o[:, b * HEAD_DIM : (b + 1) * HEAD_DIM]
        acc[:, row, :] = res
        both = jnp.where(tok == hrow, top, 0.0) + jnp.where(tok == hrow + heads, total, 0.0)
        stat[pl.ds(row, 1), :] = jnp.sum(both, axis=0, keepdims=True)

    @pl.when(step < new_steps)
    def _():
        for b in range(block):
            row = step * block + b
            page(row, new_len[row], new_ref[b, 0], new_ref[b, 1])

    @pl.when(step >= new_steps)
    def _():
        for b in range(block):
            row = step * block + b
            page(row, kept_len[row - n_new], kept_ref[b, 0], kept_ref[b, 1])

    @pl.when(step == pl.num_programs(0) - 1)
    def _():
        group = HEAD_DIM // span
        lane = lax.broadcasted_iota(i32, (rows, HEAD_DIM), 1)
        body = heads * span
        per_row = body // HEAD_DIM
        tail = out_ref.shape[1] - rows
        for k in range(ranks):
            for m in range(per_row):
                piece = jnp.zeros((rows, HEAD_DIM), f32)
                for c in range(group):
                    src = acc[m * group + c]
                    turn = (c * span - k * span) % HEAD_DIM
                    src = pltpu.roll(src, turn, 1) if turn else src
                    piece = jnp.where(lane // span == c, src, piece)
                out_ref[k, pl.ds(0, rows), pl.ds(m * HEAD_DIM, HEAD_DIM)] = piece
            out_ref[k, pl.ds(0, rows), pl.ds(body, HEAD_DIM)] = stat[...]
            out_ref[k, pl.ds(rows, tail), :] = jnp.zeros((tail, out_ref.shape[2]), f32)
            for h in range(heads):
                spot = pl.ds((h % per_row) * HEAD_DIM, HEAD_DIM)
                out_ref[k, pl.ds(rows + h // per_row, 1), spot] = own_ref[pl.ds(h, 1), :]


def attend(q_parts, own_t, kv_pool, kept, new_len, kept_len):
    ranks, rows, wide = q_parts.shape
    heads = wide // HEAD_DIM
    n_new, n_kept = kv_pool.shape[0], kept.shape[0]
    block = 4
    span = HEAD_DIM // ranks
    body = heads * span
    own_rows = heads * HEAD_DIM // body
    out_rows = -(-(rows + own_rows) // 8) * 8
    tokens, width = kv_pool.shape[2], kv_pool.shape[3]
    new_steps = n_new // block
    page = (block, 2, tokens, width)
    flops = 2 * rows * tokens * width * 16 * heads
    return pl.pallas_call(
        functools.partial(attend_kernel, n_new, n_kept, block, span),
        grid_spec=pltpu.PrefetchScalarGridSpec(
            num_scalar_prefetch=2,
            grid=((n_new + n_kept) // block,),
            in_specs=[
                pl.BlockSpec((ranks, rows, wide), lambda i, *_: (0, 0, 0)),
                pl.BlockSpec((heads, HEAD_DIM), lambda i, *_: (0, 0)),
                pl.BlockSpec(page, lambda i, *_: (jnp.minimum(i, new_steps - 1), 0, 0, 0)),
                pl.BlockSpec(page, lambda i, *_: (jnp.maximum(i - new_steps, 0), 0, 0, 0)),
            ],
            out_specs=pl.BlockSpec((ranks, out_rows, body + HEAD_DIM), lambda i, *_: (0, 0, 0)),
            scratch_shapes=[
                pltpu.VMEM((rows, heads, HEAD_DIM), f32),
                pltpu.VMEM((heads, rows, HEAD_DIM), f32),
                pltpu.VMEM((rows, HEAD_DIM), f32),
            ],
        ),
        out_shape=jax.ShapeDtypeStruct((ranks, out_rows, body + HEAD_DIM), f32),
        cost_estimate=pl.CostEstimate(flops=flops, bytes_accessed=6 << 20, transcendentals=0),
        name="attend",
    )(new_len, kept_len, q_parts, own_t, kv_pool, kept)


def combine_kernel(
    span, n_new, slot, where, new_ref, kept_ref, own_ref, val_ref, slot_ref, out_ref, top, reach, own_top
):
    ranks = kept_ref.shape[0]
    n_kept = slot_ref.shape[1] - n_new
    per = n_kept // ranks
    body = new_ref.shape[1] - HEAD_DIM
    heads = body // span
    per_row = body // HEAD_DIM
    slots = out_ref.shape[0]
    kv_rank, tp_rank = where[0], where[1]
    own_rows = own_ref.shape[1]
    own_t = own_ref[0]
    for k in range(1, ranks):
        own_t = own_t + own_ref[k]
    stacked = jnp.concatenate(
        [own_t[h // per_row : h // per_row + 1, (h % per_row) * HEAD_DIM : (h % per_row + 1) * HEAD_DIM] for h in range(heads)]
        + [jnp.zeros((HEAD_DIM - heads, HEAD_DIM), f32)],
        axis=0,
    )
    own = stacked.T
    own_top[...] = own
    top[...] = own
    stats_new = new_ref[:, body:]
    reach[pl.ds(0, n_new), :] = stats_new
    for k in range(ranks):
        reach[pl.ds(n_new + k * per, per), :] = kept_ref[k, :, body:]
    stats = reach[...]

    def grow(p, _):
        row = pl.ds(slot[p], 1)
        top[row, :] = jnp.maximum(top[row, :], reach[pl.ds(p, 1), :])
        return 0

    pages = n_new + n_kept
    for p in range(pages):
        grow(p, 0)
    for p in range(pages):
        reach[pl.ds(p, 1), :] = top[pl.ds(slot[p], 1), :]
    lane = lax.broadcasted_iota(i32, (pages, HEAD_DIM), 1)
    fade = jnp.where(lane < heads, jnp.exp(jnp.where(lane < heads, stats - reach[...], 0.0)), 0.0)
    sums = pltpu.roll(stats, HEAD_DIM - heads, 1) * fade
    hl = lax.broadcasted_iota(i32, (slots, HEAD_DIM), 1)
    own_w = jnp.where(hl < heads, jnp.exp(jnp.where(hl < heads, own_top[...] - top[...], 0.0)), 0.0)
    spread = (lax.broadcasted_iota(i32, (HEAD_DIM, body), 1) // span == lax.broadcasted_iota(i32, (HEAD_DIM, body), 0)).astype(bf16)
    member = (lax.broadcasted_iota(i32, (slots, pages), 0) == slot_ref[...]).astype(bf16)

    def by_one_hot_right(x, hot):
        return sum(jnp.dot(part, hot, preferred_element_type=f32) for part in three(x))

    def by_one_hot_left(hot, x):
        return sum(jnp.dot(hot, part, preferred_element_type=f32) for part in three(x))

    fade_wide = by_one_hot_right(fade, spread)
    body_all = jnp.concatenate([new_ref[:, :body]] + [kept_ref[k, :, :body] for k in range(ranks)], axis=0)
    weighted = by_one_hot_left(member, body_all * fade_wide)
    total = by_one_hot_left(member, sums) + own_w
    group = HEAD_DIM // span
    ratio = heads // (val_ref.shape[1] // HEAD_DIM)
    lane_s = lax.broadcasted_iota(i32, (slots, HEAD_DIM), 1)
    values = []
    for m in range(per_row):
        piece = jnp.zeros((slots, HEAD_DIM), f32)
        for c in range(group):
            h = (m * group + c) // ratio
            src = val_ref[:, h * HEAD_DIM : (h + 1) * HEAD_DIM].astype(f32)
            turn = lax.rem(c * span - kv_rank * span + HEAD_DIM, HEAD_DIM)
            piece = jnp.where(lane_s // span == c, pltpu.roll(src, turn, 1), piece)
        values.append(piece)
    values = jnp.concatenate(values, axis=1)
    own_wide = by_one_hot_right(own_w, spread)
    total_wide = by_one_hot_right(total, spread)
    attn = ((weighted + own_wide * values) / total_wide).astype(bf16)
    pairs = 2
    each = slots // (ranks * pairs)
    r = lax.broadcasted_iota(i32, (slots, slots), 0)
    half = slots // pairs
    side = r // half
    inner = r - side * half
    k_of = inner // each
    core = jnp.where(side == 0, tp_rank, 1 - tp_rank)
    source = (k_of * pairs + core) * each + (inner - k_of * each)
    turned = (lax.broadcasted_iota(i32, (slots, slots), 1) == source).astype(bf16)
    out_ref[...] = jnp.dot(turned, attn, preferred_element_type=f32).astype(bf16)


def combine(slot_all, new, kept, own, values, where, span):
    pages = slot_all.shape[0]
    slots = values.shape[0]
    body = new.shape[1] - HEAD_DIM
    return pl.pallas_call(
        functools.partial(combine_kernel, span, new.shape[0]),
        out_shape=jax.ShapeDtypeStruct((slots, body), bf16),
        in_specs=[SMEM, SMEM] + [VMEM] * 5,
        out_specs=VMEM,
        scratch_shapes=[
            pltpu.VMEM((slots, HEAD_DIM), f32),
            pltpu.VMEM((pages, HEAD_DIM), f32),
            pltpu.VMEM((slots, HEAD_DIM), f32),
        ],
        cost_estimate=pl.CostEstimate(flops=1 << 28, bytes_accessed=1 << 20, transcendentals=0),
        name="combine",
    )(slot_all, where, new, kept, own, values, slot_all[None, :])


def mlp_kernel(xa, xb, gain, wg, wu, wd, out, xn, scale, total):
    j = pl.program_id(0)
    half = xa.shape[0]

    @pl.when(j == 0)
    def _():
        for s, ref in enumerate((xa, xb)):
            x = ref[...].astype(f32)
            rows = pl.ds(s * half, half)
            scale[rows, :] = lax.rsqrt(jnp.sum(x * x, axis=1, keepdims=True) / D + norm_eps)
            xn[rows, :] = (x * gain[...]).astype(bf16)

    x = xn[...]
    s = scale[...]
    g = jnp.dot(x, wg[...], preferred_element_type=f32) * s
    u = jnp.dot(x, wu[...], preferred_element_type=f32) * s
    h = (g / (1.0 + jnp.exp(-g)) * u).astype(bf16)
    part = jnp.dot(h, wd[...], preferred_element_type=f32)

    @pl.when(j == 0)
    def _():
        total[...] = part

    @pl.when(j > 0)
    def _():
        total[...] += part

    @pl.when(j == pl.num_programs(0) - 1)
    def _():
        out[...] = total[...].astype(bf16)


def mlp(xa, xb, gain, wg, wu, wd):
    half, d = xa.shape
    ff = wg.shape[1]
    tile = 256 if ff % 256 == 0 else ff
    return pl.pallas_call(
        mlp_kernel,
        grid=(ff // tile,),
        in_specs=[
            pl.BlockSpec((half, d), lambda j: (0, 0)),
            pl.BlockSpec((half, d), lambda j: (0, 0)),
            pl.BlockSpec((1, d), lambda j: (0, 0)),
            pl.BlockSpec((d, tile), lambda j: (0, j)),
            pl.BlockSpec((d, tile), lambda j: (0, j)),
            pl.BlockSpec((tile, d), lambda j: (j, 0)),
        ],
        out_specs=pl.BlockSpec((2 * half, d), lambda j: (0, 0)),
        out_shape=jax.ShapeDtypeStruct((2 * half, d), bf16),
        scratch_shapes=[
            pltpu.VMEM((2 * half, d), bf16),
            pltpu.VMEM((2 * half, 1), f32),
            pltpu.VMEM((2 * half, d), f32),
        ],
        cost_estimate=pl.CostEstimate(flops=12 * half * d * ff, bytes_accessed=6 * d * ff, transcendentals=0),
        name="mlp",
    )(xa, xb, gain, wg, wu, wd)


def routes(new_owner, new_local, groups, ranks):
    cols = new_owner.shape[1]
    per_dev = cols // ranks
    npr, cap = per_dev // groups, per_dev // ranks
    count = groups * cols
    g_me, k_me = lax.axis_index("grp"), lax.axis_index("kv")
    own, loc = new_owner.reshape(count), new_local.reshape(count)
    y = jnp.arange(count, dtype=i32)
    g_of, k_of = y // cols, (y % cols) // per_dev
    sg, sk = own // ranks, own % ranks
    before = y[:, None] < y[None, :]
    key1 = (y // per_dev) * groups + sg
    rank_z = jnp.sum(((key1[:, None] == key1[None, :]) & before).astype(i32), axis=0)
    key2 = k_of * (groups * ranks) + own
    rank_k = jnp.sum(((key2[:, None] == key2[None, :]) & before).astype(i32), axis=0)

    def table(length, hit, spot, value):
        rows = jnp.arange(length, dtype=i32)[:, None]
        chosen = hit[None, :] & (spot[None, :] == rows)
        return jnp.sum(jnp.where(chosen, value[None, :], 0), axis=1)

    here = sg == g_me
    shift_k = (k_of - k_me + ranks) % ranks
    outgoing = table(per_dev, own == g_me * ranks + k_me, shift_k * cap + rank_k, loc)
    shift_g = (g_of - g_me + groups) % groups
    came_k = (k_me - sk + ranks) % ranks
    sorting = table(per_dev, here & (k_of == k_me), shift_g * npr + rank_z, came_k * cap + rank_k)
    came_g = (g_me - sg + groups) % groups
    placing = table(per_dev, y // per_dev == g_me * ranks + k_me, y % per_dev, came_g * npr + rank_z)
    send = sg * (ranks * npr) + k_of * npr + rank_z
    come = g_of * (ranks * npr) + k_of * npr + rank_z
    owned = sk * per_dev + loc
    send_here = lax.dynamic_slice_in_dim(send, g_me * cols, cols, 0)
    to_owner = table(cols, here, owned, come)
    from_owner = table(cols, here, come, owned)
    return outgoing, sorting, placing, send_here, to_owner, from_owner


def one_hot(idx, width):
    return (idx[:, None] == jnp.arange(width, dtype=i32)[None, :]).astype(bf16)


def pick(hot, x):
    return jnp.dot(hot, x, preferred_element_type=f32).astype(bf16)


def per_device(
    hidden_states,
    attn_gain,
    mlp_gain,
    w_query,
    w_out,
    w_gate,
    w_up,
    w_down,
    kv_pool,
    resident_cache,
    resident_slot,
    resident_len,
    new_owner,
    new_local,
    new_slot,
    new_len,
    token_kv,
):
    groups, ranks, pairs = lax.axis_size("grp"), lax.axis_size("kv"), lax.axis_size("tp")
    k_me, t_me = lax.axis_index("kv"), lax.axis_index("tp")
    slots, feat = hidden_states.shape
    per_dev, kept_dev = new_slot.shape[1], resident_slot.shape[1]
    cols = new_owner.shape[1]
    heads = w_query.shape[1] // HEAD_DIM
    kv_here = token_kv.shape[2] // HEAD_DIM
    ratio = heads // kv_here
    span = HEAD_DIM // ranks
    tokens = kv_pool.shape[2]

    outgoing, sorting, placing, send_here, to_owner, from_owner = routes(new_owner, new_local, groups, ranks)

    bounds, lo = [], 0
    for share in SHARES:
        size = int(tokens * share)
        bounds.append((lo, size))
        lo += size
    packed = [page_gather(outgoing, kv_pool, lo, size, ranks) for lo, size in bounds]

    features = hidden_states.astype(f32)
    mine = jnp.concatenate([new_slot[0], new_len[0], resident_slot[0]]).astype(f32)
    mine = jnp.pad(mine, (0, HEAD_DIM - mine.shape[0]))
    told = lax.all_gather(jnp.concatenate([mine, jnp.sum(features * features, axis=1)]), "kv")
    n_slot = told[:, :per_dev].reshape(cols)
    n_len = told[:, per_dev : 2 * per_dev].reshape(cols)
    k_slot = told[:, 2 * per_dev : 2 * per_dev + kept_dev].reshape(ranks * kept_dev).astype(i32)
    scale = lax.rsqrt(jnp.sum(told[:, HEAD_DIM:], axis=0) / D + norm_eps) * HEAD_DIM ** (-0.5)

    first = shifted([packed[0][0]] + [after(p, told) for p in packed[0][1:]], "kv")

    hot_send = send_here[None, :] == jnp.arange(cols, dtype=i32)[:, None]
    p_slot = jnp.sum(jnp.where(hot_send, n_slot[None, :], 0.0), axis=1).astype(i32)
    p_len = jnp.sum(jnp.where(hot_send, n_len[None, :], 0.0), axis=1)
    extra = jnp.stack(three(scale), axis=1)
    wide = jnp.concatenate([hidden_states, jnp.pad(extra, ((0, 0), (0, HEAD_DIM - 3)))], axis=1)
    rows = pick(one_hot(p_slot, slots), wide)
    rows = jnp.where(jnp.arange(feat + HEAD_DIM)[None, :] == feat + 3, p_len[:, None].astype(bf16), rows)
    came = lax.all_to_all(rows, "grp", 0, 0, tiled=True)
    theirs = pick(one_hot(to_owner, cols), came)
    kept_rows = pick(one_hot(k_slot, slots), wide)
    asked = jnp.concatenate(
        [theirs.reshape(ranks, per_dev, -1), kept_rows.reshape(ranks, kept_dev, -1)], axis=1
    ).reshape(ranks * (per_dev + kept_dev), -1)
    both = jnp.concatenate([asked, wide], axis=0)
    row_scale = jnp.sum(both[:, feat : feat + 3].astype(f32), axis=1)
    normed = (both[:, :feat].astype(f32) * attn_gain).astype(bf16)
    partial_query = jnp.dot(normed, w_query, preferred_element_type=f32) * row_scale[:, None]
    count = ranks * (per_dev + kept_dev)
    q_parts = lax.all_to_all(
        partial_query[:count].reshape(ranks, per_dev + kept_dev, heads * HEAD_DIM), "kv", 0, 0, tiled=True
    )
    own_q = partial_query[count:].reshape(slots, kv_here, ratio, HEAD_DIM)
    own_keys = token_kv[:, 0].astype(f32).reshape(slots, kv_here, 1, HEAD_DIM)
    own_score = jnp.sum(own_q * own_keys, axis=3).reshape(slots, heads).T
    lens = lax.dynamic_slice_in_dim(theirs[:, feat + 3], k_me * per_dev, per_dev, 0).astype(i32)

    results = attend(q_parts, own_score, kv_pool, resident_cache[0], lens, resident_len[0])
    back = lax.all_to_all(results, "kv", 0, 0, tiled=True)
    second = [shifted([p[0]] + [after(x, back) for x in p[1:]], "kv") for p in packed[1:]]
    got = jnp.take(back[:, :per_dev].reshape(cols, -1), from_owner, axis=0, mode="clip")
    home = lax.all_to_all(got, "grp", 0, 0, tiled=True)
    stage2 = [first] + second
    moved = []
    for n, parts in enumerate(stage2):
        ready = page_sort(sorting, parts, groups)
        if n:
            ready = [ready[0]] + [after(x, home) for x in ready[1:]]
        moved.append(shifted(ready, "grp"))

    own_back = back[:, per_dev + kept_dev : per_dev + kept_dev + HEAD_DIM // span, : heads * span]
    where = jnp.stack([k_me, t_me]).astype(i32)
    attn = combine(
        jnp.concatenate([p_slot, k_slot]),
        home,
        back[:, per_dev : per_dev + kept_dev],
        own_back,
        token_kv[:, 1],
        where,
        span,
    )
    branch = jnp.dot(attn, w_out.reshape(heads * span, D), preferred_element_type=f32)
    half = slots // pairs
    swap = [(i, (i + 1) % pairs) for i in range(pairs)]
    other = lax.ppermute(branch[half:].astype(bf16), "tp", swap)
    each = half // ranks
    my_rows = features.reshape(ranks, pairs, each, feat)
    my_rows = lax.dynamic_index_in_dim(my_rows, t_me, 1, False)
    laid = (branch[:half] + other.astype(f32)).reshape(ranks, each, ranks, feat)
    spot = jnp.arange(ranks, dtype=i32) == k_me
    laid = laid + jnp.where(spot[None, None, :, None], my_rows[:, :, None, :], 0.0)
    shared = lax.all_to_all(laid.reshape(ranks, each, D).astype(bf16), "kv", 0, 0, tiled=True)
    resid = jnp.sum(shared.astype(f32), axis=0).astype(bf16)
    xa = lax.all_gather(resid, "kv", tiled=True)
    xb = lax.ppermute(xa, "tp", swap)
    down = mlp(xa, xb, mlp_gain[None, :], w_gate, w_up, w_down)
    other = lax.ppermute(down[half:], "tp", swap)
    summed = (down[:half].astype(f32) + other.astype(f32)).astype(bf16)
    shared = lax.all_to_all(summed.reshape(ranks, each, D), "kv", 0, 0, tiled=True)
    mixed = (resid.astype(f32) + jnp.sum(shared.astype(f32), axis=0)).astype(bf16)

    new_pages = None
    for (lo, size), parts in zip(bounds, moved):
        new_pages = page_place(placing, parts, lo, tokens, new_pages)
    return (mixed, new_pages[None])


def solution(mesh):
    return jax.shard_map(
        per_device,
        mesh=mesh,
        in_specs=(
            P("grp", "kv"),
            P("kv"),
            P(),
            P("kv", "tp"),
            P("tp", "kv", None),
            P(None, ("kv", "tp")),
            P(None, ("kv", "tp")),
            P(("kv", "tp"), None),
            P(("grp", "kv"), None, None, "tp"),
            P("grp", "kv", None, None, "tp"),
            P("grp", "kv"),
            P("grp", "kv"),
            P(),
            P(),
            P("grp", "kv"),
            P("grp", "kv"),
            P("grp", None, "tp"),
        ),
        out_specs=(P(("grp", "kv", "tp"), None), P("grp", "kv", None, None, "tp")),
        check_vma=False,
    )
```
